32 devices in a mesh: gx: 16 (over z, y, x), gy: 2 (over core).
Axes of the slice: x: 2, y: 2, z: 4, core: 2. Of those that a mesh axis runs over, the one named last changes fastest.
Arguments:
- fields: bfloat16 [4, 1, 3072, 3072], P(None, None, 'gx', 'gy'), may hold values from -6 to 6
- x_codes: int32 [1024], replicated, may hold values from 0 to 1024, as said below
- y_codes: int32 [1020], replicated, may hold values from 0 to 1024, as said below
Outputs:
- spectrum: float32 [4, 1, 1024, 1020], P(None, None, 'gx', 'gy')
- lowpass: float32 [4, 1, 3072, 3072], P(None, None, 'gx', 'gy')
The draws below stay inside these ranges and needn't reach their ends.
Inputs may be any that keep to these rules, and one draw needn't show every extreme that they name: `x_codes`: distinct codes in rising order, each naming one real Fourier basis function with wavenumber at most 512. `y_codes`: distinct codes in rising order, each naming one real Fourier basis function with wavenumber at most 512.
All inputs are finite; a program needn't handle non-finite values.
Results may differ from the reference program's by a relative error of at most 0.006.
Values may be sent and summed in bfloat16 or wider, within the bound.
A program may use at most 64 MiB of HBM per device.

```python
import math
import jax
import jax.numpy as jnp
from jax import lax

FIELDS = 4
NX = 3072
NY = 3072
BAND = 512
KX = 1024
KY = 1020
ZW = 1


def draw_x_codes(key, part):
    shuffled = jax.random.permutation(jax.random.fold_in(key, 11), 2 * BAND + 1)
    return jnp.sort(shuffled[:KX]).astype(jnp.int32)


def draw_y_codes(key, part):
    shuffled = jax.random.permutation(jax.random.fold_in(key, 23), 2 * BAND + 1)
    return jnp.sort(shuffled[:KY]).astype(jnp.int32)


def block_scale(own_key, dims, shards, least, top_value):
    def one(dim, parts):
        heights = jax.random.uniform(jax.random.fold_in(jax.random.fold_in(own_key, 6), dim), (parts,), jnp.float32, least / len(shards), top_value / len(shards))
        return jnp.repeat(jnp.exp(heights), dims[dim] // parts).reshape((-1,) + (1,) * (len(dims) - dim - 1))

    level = one(*shards[0])
    for cut in shards[1:]:
        level = level * one(*cut)
    return level


def scatter_about(key, shape, scale, reach, split=(), kind=jnp.bfloat16):
    values = scale * jax.random.normal(key, shape, jnp.float32)
    if split:
        values = values * block_scale(key, shape, split, -0.22, 0.18)
    return jnp.clip(values, -reach, reach).astype(kind)


def setup_inputs(seed: int = 0) -> dict:
    key_of = jax.random.split(jax.random.key(seed), 4)
    fields = scatter_about(key_of[0], (FIELDS, ZW, NX, NY), 1.0, 6.0, ((2, 16), (3, 2)))
    x_codes = draw_x_codes(jax.random.fold_in(key_of[3], 71), 0)
    y_codes = draw_y_codes(jax.random.fold_in(key_of[3], 71), 0)
    return {"fields": fields, "x_codes": x_codes, "y_codes": y_codes}


def mode_table(picked, length):
    position = jnp.arange(length, dtype=jnp.int32)
    frequency = jnp.where(picked <= BAND, picked, picked - BAND).astype(jnp.int32)
    phase_index = frequency[:, None] * position[None, :] % length
    radians = phase_index.astype(jnp.float32) * (2.0 * math.pi / length)
    values = jnp.where(picked[:, None] <= BAND, jnp.cos(radians), jnp.sin(radians))
    norm_factor = jnp.where(picked == 0, 1.0 / math.sqrt(length), math.sqrt(2.0 / length)).astype(jnp.float32)
    return (values * norm_factor[:, None]).astype(jnp.bfloat16)

def reference(fields, x_codes, y_codes):
    highest = lax.Precision.HIGHEST
    x_table = mode_table(x_codes, NX).astype(jnp.float32)
    y_table = mode_table(y_codes, NY).astype(jnp.float32)
    partial_value = jnp.einsum('fzxy,ky->fzxk', fields.astype(jnp.float32), y_table, precision=highest)
    spectrum = jnp.einsum('jx,fzxk->fzjk', x_table, partial_value, precision=highest)
    coarse = spectrum.astype(jnp.bfloat16).astype(jnp.float32)
    synth_x = jnp.einsum('jx,fzjk->fzxk', x_table, coarse, precision=highest)
    lowpass = jnp.einsum('fzxk,ky->fzxy', synth_x, y_table, precision=highest)
    return (spectrum, lowpass)
```

```python
import math

import jax
import jax.numpy as jnp
from jax import lax
from jax.sharding import PartitionSpec as P

NX = 3072
NY = 3072
BAND = 512


def angle(freq, position, length):
    phase = freq[None, :] * position[:, None] % length
    return phase.astype(jnp.float32) * (2.0 * math.pi / length)


def mode_table(picked, first, amount, length, live=None):
    step = 64 if amount % 64 == 0 else 8
    freq = jnp.where(picked <= BAND, picked, picked - BAND)
    coarse_angle = angle(freq, first + step * jnp.arange(amount // step, dtype=jnp.int32), length)
    fine_angle = angle(freq, jnp.arange(step, dtype=jnp.int32), length)
    norm = jnp.where(picked == 0, 1.0 / math.sqrt(length), math.sqrt(2.0 / length)).astype(jnp.float32)
    if live is not None:
        norm = jnp.where(live, norm, 0.0)
    is_cos = (picked <= BAND)[None, :]
    c, s = jnp.cos(coarse_angle), jnp.sin(coarse_angle)
    first_part = jnp.where(is_cos, c, s) * norm[None, :]
    second_part = jnp.where(is_cos, -s, c) * norm[None, :]
    fc, fs = jnp.cos(fine_angle), jnp.sin(fine_angle)
    first_part, second_part, fc, fs = lax.optimization_barrier((first_part, second_part, fc, fs))
    table = first_part[:, None, :] * fc[None] + second_part[:, None, :] * fs[None]
    return table.astype(jnp.bfloat16).reshape(amount, picked.shape[0])


def build(gx, gy):
    def local(fields, x_codes, y_codes):
        nf, nz, x_local, y_local = fields.shape
        lead = nf * nz
        ky = y_codes.shape[0] // gy
        kx = x_codes.shape[0] // gx
        unit = 128 * gx // math.gcd(128 * gx, lead)
        if unit > 2 * ky:
            unit = gx // math.gcd(gx, lead)
        kpad = -(-ky // unit) * unit
        cols = lead * kpad // gx
        me_y = lax.axis_index("gy")
        y_first = me_y * y_local
        padded = jnp.pad(y_codes.reshape(gy, ky), ((0, 0), (0, kpad - ky)))
        live = jnp.broadcast_to(jnp.arange(kpad)[None] < ky, (gy, kpad)).reshape(-1)
        y_tab = mode_table(padded.reshape(-1), y_first, y_local, NY, live)
        x_tab = mode_table(x_codes, 0, x_local * gx, NX)
        grid = fields.reshape(lead * x_local, y_local)
        part = jnp.dot(grid, y_tab, preferred_element_type=jnp.float32).reshape(lead * x_local, gy, kpad)
        own = lax.dynamic_index_in_dim(part, me_y, 1, keepdims=False)
        for shift in range(1, gy):
            there = lax.rem(me_y + shift, gy)
            block = lax.dynamic_index_in_dim(part, there, 1, keepdims=False).astype(jnp.bfloat16)
            got = lax.ppermute(block, "gy", [(i, (i + shift) % gy) for i in range(gy)])
            own = own + got.astype(jnp.float32)
        send = own.astype(jnp.bfloat16).reshape(lead, x_local, kpad)
        if cols <= kpad:
            def spread(a):
                n = a.shape[1]
                return a.reshape(lead, n, kpad // cols, cols).transpose(0, 2, 1, 3).reshape(gx, n, cols)

            def merge(a):
                n = a.shape[1]
                return a.reshape(lead, kpad // cols, n, cols).transpose(0, 2, 1, 3).reshape(lead, n, kpad)
        else:
            def spread(a):
                n = a.shape[1]
                return a.transpose(1, 0, 2).reshape(n, gx, cols).transpose(1, 0, 2)

            def merge(a):
                n = a.shape[1]
                return a.transpose(1, 0, 2).reshape(n, lead, kpad).transpose(1, 0, 2)
        lines = lax.all_to_all(spread(send), "gx", split_axis=0, concat_axis=0, tiled=True)
        lines = lines.reshape(gx * x_local, cols)
        modes = lax.dot_general(x_tab, lines, (((0,), (0,)), ((), ())), preferred_element_type=jnp.float32)
        coarse = modes.astype(jnp.bfloat16)
        synth = jnp.dot(x_tab, coarse, preferred_element_type=jnp.float32).astype(jnp.bfloat16)
        back = lax.all_to_all(synth.reshape(gx, x_local, cols), "gx", split_axis=0, concat_axis=0, tiled=True)
        spec = lax.all_to_all(coarse.reshape(gx, kx, cols), "gx", split_axis=0, concat_axis=0, tiled=True)
        spectrum = merge(spec)[:, :, :ky].astype(jnp.float32).reshape(nf, nz, kx, ky)
        mine = merge(back).reshape(lead * x_local, kpad)
        y_parts = y_tab.reshape(y_local, gy, kpad)
        whole = jnp.zeros((gy, lead * x_local, kpad), jnp.bfloat16)
        whole = lax.dynamic_update_index_in_dim(whole, mine, me_y, 0)
        for shift in range(1, gy):
            got = lax.ppermute(mine, "gy", [(i, (i + shift) % gy) for i in range(gy)])
            whole = lax.dynamic_update_index_in_dim(whole, got, lax.rem(me_y + gy - shift, gy), 0)
        wide = whole.transpose(1, 0, 2).reshape(lead * x_local, gy * kpad)
        low = lax.dot_general(wide, y_tab, (((1,), (1,)), ((), ())), preferred_element_type=jnp.float32)
        return spectrum, low.reshape(nf, nz, x_local, y_local)

    return local


def solution(mesh):
    return jax.shard_map(
        build(mesh.shape["gx"], mesh.shape["gy"]),
        mesh=mesh,
        in_specs=(P(None, None, "gx", "gy"), P(), P()),
        out_specs=(P(None, None, "gx", "gy"), P(None, None, "gx", "gy")),
        check_vma=False,
    )
```

```python
import functools
import math

import jax
import jax.numpy as jnp
from jax import lax
from jax.experimental import pallas as pl
from jax.experimental.pallas import tpu as pltpu
from jax.sharding import PartitionSpec as P

NX = 3072
NY = 3072
BAND = 512


def angle(freq, position, length):
    phase = freq[None, :] * position[:, None] % length
    return phase.astype(jnp.float32) * (2.0 * math.pi / length)


def mode_parts(picked, first, amount, length, live=None):
    step = 64 if amount % 64 == 0 else 8
    freq = jnp.where(picked <= BAND, picked, picked - BAND)
    coarse_angle = angle(freq, first + step * jnp.arange(amount // step, dtype=jnp.int32), length)
    fine_angle = angle(freq, jnp.arange(step, dtype=jnp.int32), length)
    norm = jnp.where(picked == 0, 1.0 / math.sqrt(length), math.sqrt(2.0 / length)).astype(jnp.float32)
    if live is not None:
        norm = jnp.where(live, norm, 0.0)
    is_cos = (picked <= BAND)[None, :]
    c, s = jnp.cos(coarse_angle), jnp.sin(coarse_angle)
    first_part = jnp.where(is_cos, c, s) * norm[None, :]
    second_part = jnp.where(is_cos, -s, c) * norm[None, :]
    fc, fs = jnp.cos(fine_angle), jnp.sin(fine_angle)
    return lax.optimization_barrier((first_part, second_part, fc, fs))


def mode_table(picked, first, amount, length, live=None):
    first_part, second_part, fc, fs = mode_parts(picked, first, amount, length, live)
    table = first_part[:, None, :] * fc[None] + second_part[:, None, :] * fs[None]
    return table.astype(jnp.bfloat16).reshape(amount, picked.shape[0])


def al(v, m):
    return pl.multiple_of(v, m)


def exchange_kernel(
    gx, lead, x_local, kx, kpad, cols,
    grid_ref, y_ref, xa_ref, xb_ref, fc_ref, fs_ref, spec_ref, wide_ref,
    other, inc, part, lines, xt, acc, coarse, syn,
    gs, gr, s1, r1, s2, r2, s3, r3, s4, r4,
):
    me = lax.axis_index("gx")
    half = lax.axis_index("gy")
    peer = 1 - half
    groups = gx // lead
    my_group, my_lead = me // lead, lax.rem(me, lead)
    bf, f32 = jnp.bfloat16, jnp.float32

    barrier = pltpu.get_barrier_semaphore()
    pl.semaphore_signal(barrier, inc=1, device_id={"gy": peer})

    @pl.loop(1, gx)
    def _(t):
        pl.semaphore_signal(barrier, inc=1, device_id={"gx": lax.rem(me + t, gx)})

    def frows(f):
        return pl.ds(al(f * x_local, x_local), x_local)

    def blk(j):
        return pl.ds(al(j * x_local, x_local), x_local)

    def lanes(base, g):
        return pl.ds(al(base + g * cols, cols), cols)

    @pl.loop(0, lead)
    def _(t):
        f = lax.rem(my_lead + t, lead)
        other[frows(f), :] = jnp.dot(
            grid_ref[frows(f), :], y_ref[:, pl.ds(al(peer * kpad, kpad), kpad)], preferred_element_type=f32
        ).astype(bf)

    pl.semaphore_wait(barrier, gx)

    def swap(f):
        return pltpu.make_async_remote_copy(
            src_ref=other.at[frows(f), :], dst_ref=inc.at[frows(f), :], send_sem=gs.at[f], recv_sem=gr.at[f],
            device_id={"gy": peer})

    @pl.loop(0, lead)
    def _(t):
        swap(lax.rem(my_lead + t, lead)).start()

    def out1(j):
        f, g = lax.rem(j, lead), j // lead
        return pltpu.make_async_remote_copy(
            src_ref=part.at[frows(f), lanes(0, g)], dst_ref=lines.at[blk(me), :], send_sem=s1.at[j],
            recv_sem=r1.at[me], device_id={"gx": j})

    def in1(j):
        return pltpu.make_async_remote_copy(
            src_ref=part.at[frows(0), lanes(0, 0)], dst_ref=lines.at[blk(j), :], send_sem=s1.at[j],
            recv_sem=r1.at[j], device_id={"gx": j})

    @pl.loop(0, lead)
    def _(t):
        f = lax.rem(my_lead + t, lead)
        own = jnp.dot(
            grid_ref[frows(f), :], y_ref[:, pl.ds(al(half * kpad, kpad), kpad)], preferred_element_type=f32
        )
        swap(f).wait_recv()
        part[frows(f), :] = (own + inc[frows(f), :].astype(f32)).astype(bf)

        @pl.loop(0, groups)
        def _(u):
            g = lax.rem(my_group + u, groups)
            j = g * lead + f

            @pl.when(j != me)
            def _():
                out1(j).start()

    lines[blk(me), :] = part[frows(my_lead), lanes(0, my_group)]

    step = fc_ref.shape[0]

    @pl.loop(0, xa_ref.shape[0])
    def _(h):
        xt[pl.ds(al(h * step, step), step), :] = (
            xa_ref[pl.ds(h, 1), :] * fc_ref[...] + xb_ref[pl.ds(h, 1), :] * fs_ref[...]
        ).astype(bf)

    acc[...] = jnp.zeros_like(acc)

    @pl.loop(0, gx)
    def _(t):
        f = lax.rem(my_lead + lead - t // groups, lead)
        g = lax.rem(my_group + t, groups)
        j = g * lead + f

        @pl.when(j != me)
        def _():
            in1(j).wait_recv()

        acc[...] += jnp.dot(lines[blk(j), :].T, xt[blk(j), :], preferred_element_type=f32)

    coarse[...] = acc[...].T.astype(bf)

    def out2(j):
        return pltpu.make_async_remote_copy(
            src_ref=syn.at[blk(j), :], dst_ref=wide_ref.at[frows(my_lead), lanes(half * kpad, my_group)],
            send_sem=s2.at[j], recv_sem=r2.at[me], device_id={"gx": j})

    def in2(j):
        f, g = lax.rem(j, lead), j // lead
        return pltpu.make_async_remote_copy(
            src_ref=syn.at[blk(j), :], dst_ref=wide_ref.at[frows(f), lanes(half * kpad, g)],
            send_sem=s2.at[j], recv_sem=r2.at[j], device_id={"gx": j})

    def mrows(j):
        return pl.ds(al(j * kx, kx), kx)

    def out3(j):
        return pltpu.make_async_remote_copy(
            src_ref=coarse.at[mrows(j), :], dst_ref=spec_ref.at[mrows(my_lead), lanes(0, my_group)],
            send_sem=s3.at[j], recv_sem=r3.at[me], device_id={"gx": j})

    def in3(j):
        f, g = lax.rem(j, lead), j // lead
        return pltpu.make_async_remote_copy(
            src_ref=coarse.at[mrows(j), :], dst_ref=spec_ref.at[mrows(f), lanes(0, g)],
            send_sem=s3.at[j], recv_sem=r3.at[j], device_id={"gx": j})

    def forward(j, side):
        f, g = lax.rem(j, lead), j // lead
        place = wide_ref.at[frows(f), lanes(side * kpad, g)]
        return pltpu.make_async_remote_copy(
            src_ref=place, dst_ref=place, send_sem=s4.at[j], recv_sem=r4.at[j], device_id={"gy": peer})

    @pl.loop(1, gx)
    def _(t):
        f = lax.rem(my_lead + t // groups, lead)
        g = lax.rem(my_group + t, groups)
        j = g * lead + f
        syn[blk(j), :] = jnp.dot(xt[blk(j), :], coarse[...], preferred_element_type=f32).astype(bf)
        out2(j).start()

    wide_ref[frows(my_lead), lanes(half * kpad, my_group)] = jnp.dot(
        xt[blk(me), :], coarse[...], preferred_element_type=f32
    ).astype(bf)
    spec_ref[mrows(my_lead), lanes(0, my_group)] = coarse[mrows(me), :]

    @pl.loop(1, gx)
    def _(t):
        out3(lax.rem(me + t, gx)).start()

    forward(me, half).start()

    @pl.loop(1, gx)
    def _(t):
        f = lax.rem(my_lead + lead - t // groups, lead)
        g = lax.rem(my_group + t, groups)
        j = g * lead + f
        in2(j).wait_recv()
        forward(j, half).start()

    @pl.loop(0, lead)
    def _(f):
        swap(f).wait_send()

    @pl.loop(1, gx)
    def _(t):
        j = lax.rem(me + t, gx)
        in3(j).wait_recv()
        out1(j).wait_send()
        out2(j).wait_send()
        out3(j).wait_send()

    @pl.loop(0, gx)
    def _(j):
        forward(j, peer).wait_recv()
        forward(j, half).wait_send()


def exchange(gx, lead, x_local, kx, kpad, cols, grid, y_tab, x_parts):
    bf, f32 = jnp.bfloat16, jnp.float32
    rows, codes = lead * x_local, gx * kx
    dma = pltpu.SemaphoreType.DMA
    vmem = pl.BlockSpec(memory_space=pltpu.VMEM)
    return pl.pallas_call(
        functools.partial(exchange_kernel, gx, lead, x_local, kx, kpad, cols),
        out_shape=(
            jax.ShapeDtypeStruct((lead * kx, kpad), bf),
            jax.ShapeDtypeStruct((rows, 2 * kpad), bf),
        ),
        in_specs=[vmem] * 6,
        out_specs=(vmem, vmem),
        scratch_shapes=[
            pltpu.VMEM((rows, kpad), bf),
            pltpu.VMEM((rows, kpad), bf),
            pltpu.VMEM((rows, kpad), bf),
            pltpu.VMEM((gx * x_local, cols), bf),
            pltpu.VMEM((gx * x_local, codes), bf),
            pltpu.VMEM((cols, codes), f32),
            pltpu.VMEM((codes, cols), bf),
            pltpu.VMEM((gx * x_local, cols), bf),
            dma((lead,)), dma((lead,)),
        ] + [dma((gx,))] * 8,
        compiler_params=pltpu.CompilerParams(
            collective_id=0, has_side_effects=True, vmem_limit_bytes=48 * 1024 * 1024
        ),
    )(grid, y_tab, *x_parts)


def build(gx, gy):
    def local(fields, x_codes, y_codes):
        nf, nz, x_local, y_local = fields.shape
        lead = nf * nz
        ky = y_codes.shape[0] // gy
        kx = x_codes.shape[0] // gx
        unit = 128 * gx // math.gcd(128 * gx, lead)
        if unit > 2 * ky:
            unit = gx // math.gcd(gx, lead)
        kpad = -(-ky // unit) * unit
        cols = lead * kpad // gx
        me_y = lax.axis_index("gy")
        y_first = me_y * y_local
        padded = jnp.pad(y_codes.reshape(gy, ky), ((0, 0), (0, kpad - ky)))
        live = jnp.broadcast_to(jnp.arange(kpad)[None] < ky, (gy, kpad)).reshape(-1)
        y_tab = mode_table(padded.reshape(-1), y_first, y_local, NY, live)
        grid = fields.reshape(lead * x_local, y_local)
        if gy == 2 and cols % 128 == 0 and cols <= kpad and kpad // cols == gx // lead and x_local % 64 == 0 and kx % 16 == 0:
            x_parts = mode_parts(x_codes, 0, x_local * gx, NX)
            spec, wide = exchange(gx, lead, x_local, kx, kpad, cols, grid, y_tab, x_parts)
            low = lax.dot_general(wide, y_tab, (((1,), (1,)), ((), ())), preferred_element_type=jnp.float32)
            spectrum = spec.astype(jnp.float32)[:, :ky].reshape(nf, nz, kx, ky)
            return spectrum, low.reshape(nf, nz, x_local, y_local)
        x_tab = mode_table(x_codes, 0, x_local * gx, NX)
        part = jnp.dot(grid, y_tab, preferred_element_type=jnp.float32).reshape(lead * x_local, gy, kpad)
        own = lax.dynamic_index_in_dim(part, me_y, 1, keepdims=False)
        for shift in range(1, gy):
            there = lax.rem(me_y + shift, gy)
            block = lax.dynamic_index_in_dim(part, there, 1, keepdims=False).astype(jnp.bfloat16)
            got = lax.ppermute(block, "gy", [(i, (i + shift) % gy) for i in range(gy)])
            own = own + got.astype(jnp.float32)
        send = own.astype(jnp.bfloat16).reshape(lead, x_local, kpad)
        if cols <= kpad:
            def spread(a):
                n = a.shape[1]
                return a.reshape(lead, n, kpad // cols, cols).transpose(0, 2, 1, 3).reshape(gx, n, cols)

            def merge(a):
                n = a.shape[1]
                return a.reshape(lead, kpad // cols, n, cols).transpose(0, 2, 1, 3).reshape(lead, n, kpad)
        else:
            def spread(a):
                n = a.shape[1]
                return a.transpose(1, 0, 2).reshape(n, gx, cols).transpose(1, 0, 2)

            def merge(a):
                n = a.shape[1]
                return a.transpose(1, 0, 2).reshape(n, lead, kpad).transpose(1, 0, 2)
        lines = lax.all_to_all(spread(send), "gx", split_axis=0, concat_axis=0, tiled=True)
        lines = lines.reshape(gx * x_local, cols)
        modes = lax.dot_general(x_tab, lines, (((0,), (0,)), ((), ())), preferred_element_type=jnp.float32)
        coarse = modes.astype(jnp.bfloat16)
        synth = jnp.dot(x_tab, coarse, preferred_element_type=jnp.float32).astype(jnp.bfloat16)
        back = lax.all_to_all(synth.reshape(gx, x_local, cols), "gx", split_axis=0, concat_axis=0, tiled=True)
        spec = lax.all_to_all(coarse.reshape(gx, kx, cols), "gx", split_axis=0, concat_axis=0, tiled=True)
        spectrum = merge(spec)[:, :, :ky].astype(jnp.float32).reshape(nf, nz, kx, ky)
        mine = merge(back).reshape(lead * x_local, kpad)
        y_parts = y_tab.reshape(y_local, gy, kpad)
        whole = jnp.zeros((gy, lead * x_local, kpad), jnp.bfloat16)
        whole = lax.dynamic_update_index_in_dim(whole, mine, me_y, 0)
        for shift in range(1, gy):
            got = lax.ppermute(mine, "gy", [(i, (i + shift) % gy) for i in range(gy)])
            whole = lax.dynamic_update_index_in_dim(whole, got, lax.rem(me_y + gy - shift, gy), 0)
        wide = whole.transpose(1, 0, 2).reshape(lead * x_local, gy * kpad)
        low = lax.dot_general(wide, y_tab, (((1,), (1,)), ((), ())), preferred_element_type=jnp.float32)
        return spectrum, low.reshape(nf, nz, x_local, y_local)

    return local


def solution(mesh):
    return jax.shard_map(
        build(mesh.shape["gx"], mesh.shape["gy"]),
        mesh=mesh,
        in_specs=(P(None, None, "gx", "gy"), P(), P()),
        out_specs=(P(None, None, "gx", "gy"), P(None, None, "gx", "gy")),
        check_vma=False,
    )
```

```python
import functools
import math

import jax
import jax.numpy as jnp
from jax import lax
from jax.experimental import pallas as pl
from jax.experimental.pallas import tpu as pltpu
from jax.sharding import PartitionSpec as P

NX = 3072
NY = 3072
BAND = 512
STEP = 64


def angle(freq, position, length):
    phase = freq[None, :] * position[:, None] % length
    return phase.astype(jnp.float32) * (2.0 * math.pi / length)


def mode_parts(picked, first, amount, length, live=None):
    step = 64 if amount % 64 == 0 else 8
    freq = jnp.where(picked <= BAND, picked, picked - BAND)
    coarse_angle = angle(freq, first + step * jnp.arange(amount // step, dtype=jnp.int32), length)
    fine_angle = angle(freq, jnp.arange(step, dtype=jnp.int32), length)
    norm = jnp.where(picked == 0, 1.0 / math.sqrt(length), math.sqrt(2.0 / length)).astype(jnp.float32)
    if live is not None:
        norm = jnp.where(live, norm, 0.0)
    is_cos = (picked <= BAND)[None, :]
    c, s = jnp.cos(coarse_angle), jnp.sin(coarse_angle)
    first_part = jnp.where(is_cos, c, s) * norm[None, :]
    second_part = jnp.where(is_cos, -s, c) * norm[None, :]
    fc, fs = jnp.cos(fine_angle), jnp.sin(fine_angle)
    return lax.optimization_barrier((first_part, second_part, fc, fs))


def mode_table(picked, first, amount, length, live=None):
    first_part, second_part, fc, fs = mode_parts(picked, first, amount, length, live)
    table = first_part[:, None, :] * fc[None] + second_part[:, None, :] * fs[None]
    return table.astype(jnp.bfloat16).reshape(amount, picked.shape[0])


def al(v, m):
    return pl.multiple_of(v, m)


def turn(freq, position, shift, length):
    product = freq * position
    quarter = jnp.floor(product * (4.0 / length) + 0.5)
    x = (product * 4.0 - quarter * length) * (2.0 * math.pi / (4 * length))
    x2 = x * x
    s = x + x * x2 * (-1 / 6 + x2 * (1 / 120 + x2 * (-1 / 5040 + x2 * (1 / 362880))))
    c = 1.0 + x2 * (-0.5 + x2 * (1 / 24 + x2 * (-1 / 720 + x2 * (1 / 40320))))
    quarter = quarter - shift
    q = quarter - 4.0 * jnp.floor(quarter * 0.25)
    odd = (q == 1.0) | (q == 3.0)
    cos_value, sin_value = jnp.where(odd, s, c), jnp.where(odd, c, s)
    cos_value = jnp.where((q == 1.0) | (q == 2.0), -cos_value, cos_value)
    return cos_value, jnp.where(q >= 2.0, -sin_value, sin_value)


def make_table(code_ref, first, length, table, ta, tb, fc, fs):
    amount, codes = table.shape
    f32 = jnp.float32
    code = code_ref[...]
    freq = jnp.where(code <= BAND, code, code - BAND).astype(f32)
    shift = jnp.where(code <= BAND, 0, 1).astype(f32)
    norm = jnp.where(code == 0, 1.0 / math.sqrt(length), math.sqrt(2.0 / length)).astype(f32)
    norm = jnp.where(code < 0, 0.0, norm)
    row = lax.broadcasted_iota(jnp.int32, (8, codes), 0)

    @pl.loop(0, amount // STEP // 8)
    def _(i):
        c, s = turn(freq, (first + (row + i * 8) * STEP).astype(f32), shift, length)
        ta[pl.ds(al(i * 8, 8), 8), :] = c * norm
        tb[pl.ds(al(i * 8, 8), 8), :] = s * norm

    @pl.loop(0, STEP // 8)
    def _(i):
        c, s = turn(freq, (row + i * 8).astype(f32), 0.0, length)
        fc[pl.ds(al(i * 8, 8), 8), :] = c
        fs[pl.ds(al(i * 8, 8), 8), :] = s

    @pl.loop(0, amount // STEP)
    def _(h):
        table[pl.ds(al(h * STEP, STEP), STEP), :] = (
            ta[pl.ds(h, 1), :] * fc[...] - tb[pl.ds(h, 1), :] * fs[...]
        ).astype(jnp.bfloat16)


def exchange_kernel(
    gx, lead, x_local, kx, kpad, cols,
    grid_ref, xcode_ref, ycode_ref, spec_ref, wide_ref, y_out,
    y_ref, ta, tb, fc, fs, other, inc, part, lines, xt, acc, coarse, syn,
    gs, gr, s1, r1, s2, r2, s3, r3, s4, r4, y_sem,
):
    me = lax.axis_index("gx")
    half = lax.axis_index("gy")
    peer = 1 - half
    groups = gx // lead
    my_group, my_lead = me // lead, lax.rem(me, lead)
    bf, f32 = jnp.bfloat16, jnp.float32

    barrier = pltpu.get_barrier_semaphore()
    pl.semaphore_signal(barrier, inc=1, device_id={"gy": peer})

    @pl.loop(1, gx)
    def _(t):
        pl.semaphore_signal(barrier, inc=1, device_id={"gx": lax.rem(me + t, gx)})

    def frows(f):
        return pl.ds(al(f * x_local, x_local), x_local)

    def blk(j):
        return pl.ds(al(j * x_local, x_local), x_local)

    def lanes(base, g):
        return pl.ds(al(base + g * cols, cols), cols)

    make_table(ycode_ref, half * y_ref.shape[0], NY, y_ref, ta, tb, fc, fs)
    y_copy = pltpu.make_async_copy(y_ref, y_out, y_sem)
    y_copy.start()

    @pl.loop(0, lead)
    def _(t):
        f = lax.rem(my_lead + t, lead)
        other[frows(f), :] = jnp.dot(
            grid_ref[frows(f), :], y_ref[:, pl.ds(al(peer * kpad, kpad), kpad)], preferred_element_type=f32
        ).astype(bf)

    pl.semaphore_wait(barrier, gx)

    def swap(f):
        return pltpu.make_async_remote_copy(
            src_ref=other.at[frows(f), :], dst_ref=inc.at[frows(f), :], send_sem=gs.at[f], recv_sem=gr.at[f],
            device_id={"gy": peer})

    @pl.loop(0, lead)
    def _(t):
        swap(lax.rem(my_lead + t, lead)).start()

    def out1(j):
        f, g = lax.rem(j, lead), j // lead
        return pltpu.make_async_remote_copy(
            src_ref=part.at[frows(f), lanes(0, g)], dst_ref=lines.at[blk(me), :], send_sem=s1.at[j],
            recv_sem=r1.at[me], device_id={"gx": j})

    def in1(j):
        return pltpu.make_async_remote_copy(
            src_ref=part.at[frows(0), lanes(0, 0)], dst_ref=lines.at[blk(j), :], send_sem=s1.at[j],
            recv_sem=r1.at[j], device_id={"gx": j})

    @pl.loop(0, lead)
    def _(t):
        f = lax.rem(my_lead + t, lead)
        own = jnp.dot(
            grid_ref[frows(f), :], y_ref[:, pl.ds(al(half * kpad, kpad), kpad)], preferred_element_type=f32
        )
        swap(f).wait_recv()
        part[frows(f), :] = (own + inc[frows(f), :].astype(f32)).astype(bf)

        @pl.loop(0, groups)
        def _(u):
            g = lax.rem(my_group + u, groups)
            j = g * lead + f

            @pl.when(j != me)
            def _():
                out1(j).start()

    lines[blk(me), :] = part[frows(my_lead), lanes(0, my_group)]

    make_table(xcode_ref, 0, NX, xt, ta, tb, fc, fs)
    acc[...] = jnp.zeros_like(acc)

    @pl.loop(0, gx)
    def _(t):
        f = lax.rem(my_lead + lead - t // groups, lead)
        g = lax.rem(my_group + t, groups)
        j = g * lead + f

        @pl.when(j != me)
        def _():
            in1(j).wait_recv()

        acc[...] += jnp.dot(lines[blk(j), :].T, xt[blk(j), :], preferred_element_type=f32)

    coarse[...] = acc[...].T.astype(bf)

    def out2(j):
        return pltpu.make_async_remote_copy(
            src_ref=syn.at[blk(j), :], dst_ref=wide_ref.at[frows(my_lead), lanes(half * kpad, my_group)],
            send_sem=s2.at[j], recv_sem=r2.at[me], device_id={"gx": j})

    def in2(j):
        f, g = lax.rem(j, lead), j // lead
        return pltpu.make_async_remote_copy(
            src_ref=syn.at[blk(j), :], dst_ref=wide_ref.at[frows(f), lanes(half * kpad, g)],
            send_sem=s2.at[j], recv_sem=r2.at[j], device_id={"gx": j})

    def mrows(j):
        return pl.ds(al(j * kx, kx), kx)

    def out3(j):
        return pltpu.make_async_remote_copy(
            src_ref=coarse.at[mrows(j), :], dst_ref=spec_ref.at[mrows(my_lead), lanes(0, my_group)],
            send_sem=s3.at[j], recv_sem=r3.at[me], device_id={"gx": j})

    def in3(j):
        f, g = lax.rem(j, lead), j // lead
        return pltpu.make_async_remote_copy(
            src_ref=coarse.at[mrows(j), :], dst_ref=spec_ref.at[mrows(f), lanes(0, g)],
            send_sem=s3.at[j], recv_sem=r3.at[j], device_id={"gx": j})

    def forward(j, side):
        f, g = lax.rem(j, lead), j // lead
        place = wide_ref.at[frows(f), lanes(side * kpad, g)]
        return pltpu.make_async_remote_copy(
            src_ref=place, dst_ref=place, send_sem=s4.at[j], recv_sem=r4.at[j], device_id={"gy": peer})

    @pl.loop(1, gx)
    def _(t):
        f = lax.rem(my_lead + t // groups, lead)
        g = lax.rem(my_group + t, groups)
        j = g * lead + f
        syn[blk(j), :] = jnp.dot(xt[blk(j), :], coarse[...], preferred_element_type=f32).astype(bf)
        out2(j).start()

    wide_ref[frows(my_lead), lanes(half * kpad, my_group)] = jnp.dot(
        xt[blk(me), :], coarse[...], preferred_element_type=f32
    ).astype(bf)
    spec_ref[mrows(my_lead), lanes(0, my_group)] = coarse[mrows(me), :]

    @pl.loop(1, gx)
    def _(t):
        out3(lax.rem(me + t, gx)).start()

    forward(me, half).start()

    @pl.loop(1, gx)
    def _(t):
        f = lax.rem(my_lead + lead - t // groups, lead)
        g = lax.rem(my_group + t, groups)
        j = g * lead + f
        in2(j).wait_recv()
        forward(j, half).start()

    y_copy.wait()

    @pl.loop(0, lead)
    def _(f):
        swap(f).wait_send()

    @pl.loop(1, gx)
    def _(t):
        j = lax.rem(me + t, gx)
        in3(j).wait_recv()
        out1(j).wait_send()
        out2(j).wait_send()
        out3(j).wait_send()

    @pl.loop(0, gx)
    def _(j):
        forward(j, peer).wait_recv()
        forward(j, half).wait_send()


def exchange(gx, lead, x_local, kx, kpad, cols, grid, x_codes, y_codes):
    bf, f32 = jnp.bfloat16, jnp.float32
    rows, codes = lead * x_local, gx * kx
    dma = pltpu.SemaphoreType.DMA
    vmem = pl.BlockSpec(memory_space=pltpu.VMEM)
    y_local = grid.shape[1]
    tall = max(gx * x_local, y_local) // STEP
    return pl.pallas_call(
        functools.partial(exchange_kernel, gx, lead, x_local, kx, kpad, cols),
        out_shape=(
            jax.ShapeDtypeStruct((lead * kx, kpad), bf),
            jax.ShapeDtypeStruct((rows, 2 * kpad), bf),
            jax.ShapeDtypeStruct((y_local, 2 * kpad), bf),
        ),
        in_specs=[vmem] * 3,
        out_specs=(vmem, vmem, pl.BlockSpec(memory_space=pl.ANY)),
        scratch_shapes=[
            pltpu.VMEM((y_local, 2 * kpad), bf),
            pltpu.VMEM((tall, codes), f32),
            pltpu.VMEM((tall, codes), f32),
            pltpu.VMEM((STEP, codes), f32),
            pltpu.VMEM((STEP, codes), f32),
            pltpu.VMEM((rows, kpad), bf),
            pltpu.VMEM((rows, kpad), bf),
            pltpu.VMEM((rows, kpad), bf),
            pltpu.VMEM((gx * x_local, cols), bf),
            pltpu.VMEM((gx * x_local, codes), bf),
            pltpu.VMEM((cols, codes), f32),
            pltpu.VMEM((codes, cols), bf),
            pltpu.VMEM((gx * x_local, cols), bf),
            dma((lead,)), dma((lead,)),
        ] + [dma((gx,))] * 8 + [dma],
        compiler_params=pltpu.CompilerParams(
            collective_id=0, has_side_effects=True, vmem_limit_bytes=48 * 1024 * 1024
        ),
    )(grid, x_codes, y_codes)


def build(gx, gy):
    def local(fields, x_codes, y_codes):
        nf, nz, x_local, y_local = fields.shape
        lead = nf * nz
        ky = y_codes.shape[0] // gy
        kx = x_codes.shape[0] // gx
        unit = 128 * gx // math.gcd(128 * gx, lead)
        if unit > 2 * ky:
            unit = gx // math.gcd(gx, lead)
        kpad = -(-ky // unit) * unit
        cols = lead * kpad // gx
        me_y = lax.axis_index("gy")
        y_first = me_y * y_local
        padded = jnp.pad(y_codes.reshape(gy, ky), ((0, 0), (0, kpad - ky)))
        live = jnp.broadcast_to(jnp.arange(kpad)[None] < ky, (gy, kpad)).reshape(-1)
        y_tab = mode_table(padded.reshape(-1), y_first, y_local, NY, live)
        grid = fields.reshape(lead * x_local, y_local)
        if gy == 2 and cols % 128 == 0 and cols <= kpad and kpad // cols == gx // lead and x_local % (8 * STEP // gx) == 0 and y_local % (8 * STEP) == 0 and kx % 16 == 0 and gx * kx == gy * kpad:
            padded = jnp.pad(y_codes.reshape(gy, ky), ((0, 0), (0, kpad - ky)), constant_values=-1)
            spec, wide, y_tab = exchange(
                gx, lead, x_local, kx, kpad, cols, grid, x_codes.reshape(1, -1), padded.reshape(1, -1)
            )
            low = lax.dot_general(wide, y_tab, (((1,), (1,)), ((), ())), preferred_element_type=jnp.float32)
            spectrum = spec.astype(jnp.float32)[:, :ky].reshape(nf, nz, kx, ky)
            return spectrum, low.reshape(nf, nz, x_local, y_local)
        x_tab = mode_table(x_codes, 0, x_local * gx, NX)
        part = jnp.dot(grid, y_tab, preferred_element_type=jnp.float32).reshape(lead * x_local, gy, kpad)
        own = lax.dynamic_index_in_dim(part, me_y, 1, keepdims=False)
        for shift in range(1, gy):
            there = lax.rem(me_y + shift, gy)
            block = lax.dynamic_index_in_dim(part, there, 1, keepdims=False).astype(jnp.bfloat16)
            got = lax.ppermute(block, "gy", [(i, (i + shift) % gy) for i in range(gy)])
            own = own + got.astype(jnp.float32)
        send = own.astype(jnp.bfloat16).reshape(lead, x_local, kpad)
        if cols <= kpad:
            def spread(a):
                n = a.shape[1]
                return a.reshape(lead, n, kpad // cols, cols).transpose(0, 2, 1, 3).reshape(gx, n, cols)

            def merge(a):
                n = a.shape[1]
                return a.reshape(lead, kpad // cols, n, cols).transpose(0, 2, 1, 3).reshape(lead, n, kpad)
        else:
            def spread(a):
                n = a.shape[1]
                return a.transpose(1, 0, 2).reshape(n, gx, cols).transpose(1, 0, 2)

            def merge(a):
                n = a.shape[1]
                return a.transpose(1, 0, 2).reshape(n, lead, kpad).transpose(1, 0, 2)
        lines = lax.all_to_all(spread(send), "gx", split_axis=0, concat_axis=0, tiled=True)
        lines = lines.reshape(gx * x_local, cols)
        modes = lax.dot_general(x_tab, lines, (((0,), (0,)), ((), ())), preferred_element_type=jnp.float32)
        coarse = modes.astype(jnp.bfloat16)
        synth = jnp.dot(x_tab, coarse, preferred_element_type=jnp.float32).astype(jnp.bfloat16)
        back = lax.all_to_all(synth.reshape(gx, x_local, cols), "gx", split_axis=0, concat_axis=0, tiled=True)
        spec = lax.all_to_all(coarse.reshape(gx, kx, cols), "gx", split_axis=0, concat_axis=0, tiled=True)
        spectrum = merge(spec)[:, :, :ky].astype(jnp.float32).reshape(nf, nz, kx, ky)
        mine = merge(back).reshape(lead * x_local, kpad)
        y_parts = y_tab.reshape(y_local, gy, kpad)
        whole = jnp.zeros((gy, lead * x_local, kpad), jnp.bfloat16)
        whole = lax.dynamic_update_index_in_dim(whole, mine, me_y, 0)
        for shift in range(1, gy):
            got = lax.ppermute(mine, "gy", [(i, (i + shift) % gy) for i in range(gy)])
            whole = lax.dynamic_update_index_in_dim(whole, got, lax.rem(me_y + gy - shift, gy), 0)
        wide = whole.transpose(1, 0, 2).reshape(lead * x_local, gy * kpad)
        low = lax.dot_general(wide, y_tab, (((1,), (1,)), ((), ())), preferred_element_type=jnp.float32)
        return spectrum, low.reshape(nf, nz, x_local, y_local)

    return local


def solution(mesh):
    return jax.shard_map(
        build(mesh.shape["gx"], mesh.shape["gy"]),
        mesh=mesh,
        in_specs=(P(None, None, "gx", "gy"), P(), P()),
        out_specs=(P(None, None, "gx", "gy"), P(None, None, "gx", "gy")),
        check_vma=False,
    )
```

```python
import functools
import math

import jax
import jax.numpy as jnp
from jax import lax
from jax.experimental import pallas as pl
from jax.experimental.pallas import tpu as pltpu
from jax.sharding import PartitionSpec as P

NX = 3072
NY = 3072
BAND = 512
STEP = 64


def angle(freq, position, length):
    phase = freq[None, :] * position[:, None] % length
    return phase.astype(jnp.float32) * (2.0 * math.pi / length)


def mode_parts(picked, first, amount, length, live=None):
    step = 64 if amount % 64 == 0 else 8
    freq = jnp.where(picked <= BAND, picked, picked - BAND)
    coarse_angle = angle(freq, first + step * jnp.arange(amount // step, dtype=jnp.int32), length)
    fine_angle = angle(freq, jnp.arange(step, dtype=jnp.int32), length)
    norm = jnp.where(picked == 0, 1.0 / math.sqrt(length), math.sqrt(2.0 / length)).astype(jnp.float32)
    if live is not None:
        norm = jnp.where(live, norm, 0.0)
    is_cos = (picked <= BAND)[None, :]
    c, s = jnp.cos(coarse_angle), jnp.sin(coarse_angle)
    first_part = jnp.where(is_cos, c, s) * norm[None, :]
    second_part = jnp.where(is_cos, -s, c) * norm[None, :]
    fc, fs = jnp.cos(fine_angle), jnp.sin(fine_angle)
    return lax.optimization_barrier((first_part, second_part, fc, fs))


def mode_table(picked, first, amount, length, live=None):
    first_part, second_part, fc, fs = mode_parts(picked, first, amount, length, live)
    table = first_part[:, None, :] * fc[None] + second_part[:, None, :] * fs[None]
    return table.astype(jnp.bfloat16).reshape(amount, picked.shape[0])


def al(v, m):
    return pl.multiple_of(v, m)


def turn(freq, position, shift, length):
    product = freq * position
    quarter = jnp.floor(product * (4.0 / length) + 0.5)
    x = (product * 4.0 - quarter * length) * (2.0 * math.pi / (4 * length))
    x2 = x * x
    s = x + x * x2 * (-1 / 6 + x2 * (1 / 120 + x2 * (-1 / 5040 + x2 * (1 / 362880))))
    c = 1.0 + x2 * (-0.5 + x2 * (1 / 24 + x2 * (-1 / 720 + x2 * (1 / 40320))))
    quarter = quarter - shift
    q = quarter - 4.0 * jnp.floor(quarter * 0.25)
    odd = (q == 1.0) | (q == 3.0)
    cos_value, sin_value = jnp.where(odd, s, c), jnp.where(odd, c, s)
    cos_value = jnp.where((q == 1.0) | (q == 2.0), -cos_value, cos_value)
    return cos_value, jnp.where(q >= 2.0, -sin_value, sin_value)


def make_table(code_ref, first, length, table, ta, tb, fc, fs):
    amount, codes = table.shape
    f32 = jnp.float32
    code = code_ref[...]
    freq = jnp.where(code <= BAND, code, code - BAND).astype(f32)
    shift = jnp.where(code <= BAND, 0, 1).astype(f32)
    norm = jnp.where(code == 0, 1.0 / math.sqrt(length), math.sqrt(2.0 / length)).astype(f32)
    norm = jnp.where(code < 0, 0.0, norm)
    row = lax.broadcasted_iota(jnp.int32, (8, codes), 0)

    @pl.loop(0, amount // STEP // 8)
    def _(i):
        c, s = turn(freq, (first + (row + i * 8) * STEP).astype(f32), shift, length)
        ta[pl.ds(al(i * 8, 8), 8), :] = c * norm
        tb[pl.ds(al(i * 8, 8), 8), :] = s * norm

    @pl.loop(0, STEP // 8)
    def _(i):
        c, s = turn(freq, (row + i * 8).astype(f32), 0.0, length)
        fc[pl.ds(al(i * 8, 8), 8), :] = c
        fs[pl.ds(al(i * 8, 8), 8), :] = s

    @pl.loop(0, amount // STEP)
    def _(h):
        table[pl.ds(al(h * STEP, STEP), STEP), :] = (
            ta[pl.ds(h, 1), :] * fc[...] - tb[pl.ds(h, 1), :] * fs[...]
        ).astype(jnp.bfloat16)


def exchange_kernel(
    gx, lead, x_local, kx, kpad, cols,
    grid_in, xcode_ref, ycode_ref, spec_ref, low_out,
    grid_ref, wide_ref, low_ref, y_ref, ta, tb, fc, fs, other, inc, part, lines, xt, acc, coarse, syn,
    gs, gr, s1, r1, s2, r2, s3, r3, s4, r4, grid_sem, low_sem,
):
    me = lax.axis_index("gx")
    half = lax.axis_index("gy")
    peer = 1 - half
    groups = gx // lead
    my_group, my_lead = me // lead, lax.rem(me, lead)
    bf, f32 = jnp.bfloat16, jnp.float32

    grid_copy = pltpu.make_async_copy(grid_in, grid_ref, grid_sem)
    grid_copy.start()
    barrier = pltpu.get_barrier_semaphore()
    pl.semaphore_signal(barrier, inc=1, device_id={"gy": peer})

    @pl.loop(1, gx)
    def _(t):
        pl.semaphore_signal(barrier, inc=1, device_id={"gx": lax.rem(me + t, gx)})

    def frows(f):
        return pl.ds(al(f * x_local, x_local), x_local)

    def blk(j):
        return pl.ds(al(j * x_local, x_local), x_local)

    def lanes(base, g):
        return pl.ds(al(base + g * cols, cols), cols)

    make_table(ycode_ref, half * y_ref.shape[0], NY, y_ref, ta, tb, fc, fs)
    grid_copy.wait()

    @pl.loop(0, lead)
    def _(t):
        f = lax.rem(my_lead + t, lead)
        other[frows(f), :] = jnp.dot(
            grid_ref[frows(f), :], y_ref[:, pl.ds(al(peer * kpad, kpad), kpad)], preferred_element_type=f32
        ).astype(bf)

    pl.semaphore_wait(barrier, gx)

    def swap(f):
        return pltpu.make_async_remote_copy(
            src_ref=other.at[frows(f), :], dst_ref=inc.at[frows(f), :], send_sem=gs.at[f], recv_sem=gr.at[f],
            device_id={"gy": peer})

    @pl.loop(0, lead)
    def _(t):
        swap(lax.rem(my_lead + t, lead)).start()

    def out1(j):
        f, g = lax.rem(j, lead), j // lead
        return pltpu.make_async_remote_copy(
            src_ref=part.at[frows(f), lanes(0, g)], dst_ref=lines.at[blk(me), :], send_sem=s1.at[j],
            recv_sem=r1.at[me], device_id={"gx": j})

    def in1(j):
        return pltpu.make_async_remote_copy(
            src_ref=part.at[frows(0), lanes(0, 0)], dst_ref=lines.at[blk(j), :], send_sem=s1.at[j],
            recv_sem=r1.at[j], device_id={"gx": j})

    @pl.loop(0, lead)
    def _(t):
        f = lax.rem(my_lead + t, lead)
        own = jnp.dot(
            grid_ref[frows(f), :], y_ref[:, pl.ds(al(half * kpad, kpad), kpad)], preferred_element_type=f32
        )
        swap(f).wait_recv()
        part[frows(f), :] = (own + inc[frows(f), :].astype(f32)).astype(bf)

        @pl.loop(0, groups)
        def _(u):
            g = lax.rem(my_group + u, groups)
            j = g * lead + f

            @pl.when(j != me)
            def _():
                out1(j).start()

    lines[blk(me), :] = part[frows(my_lead), lanes(0, my_group)]

    make_table(xcode_ref, 0, NX, xt, ta, tb, fc, fs)
    acc[...] = jnp.zeros_like(acc)

    @pl.loop(0, gx)
    def _(t):
        f = lax.rem(my_lead + lead - t // groups, lead)
        g = lax.rem(my_group + t, groups)
        j = g * lead + f

        @pl.when(j != me)
        def _():
            in1(j).wait_recv()

        acc[...] += jnp.dot(lines[blk(j), :].T, xt[blk(j), :], preferred_element_type=f32)

    coarse[...] = acc[...].T.astype(bf)

    def out2(j):
        return pltpu.make_async_remote_copy(
            src_ref=syn.at[blk(j), :], dst_ref=wide_ref.at[frows(my_lead), lanes(half * kpad, my_group)],
            send_sem=s2.at[j], recv_sem=r2.at[me], device_id={"gx": j})

    def in2(j):
        f, g = lax.rem(j, lead), j // lead
        return pltpu.make_async_remote_copy(
            src_ref=syn.at[blk(j), :], dst_ref=wide_ref.at[frows(f), lanes(half * kpad, g)],
            send_sem=s2.at[j], recv_sem=r2.at[j], device_id={"gx": j})

    def mrows(j):
        return pl.ds(al(j * kx, kx), kx)

    def out3(j):
        return pltpu.make_async_remote_copy(
            src_ref=coarse.at[mrows(j), :], dst_ref=spec_ref.at[mrows(my_lead), lanes(0, my_group)],
            send_sem=s3.at[j], recv_sem=r3.at[me], device_id={"gx": j})

    def in3(j):
        f, g = lax.rem(j, lead), j // lead
        return pltpu.make_async_remote_copy(
            src_ref=coarse.at[mrows(j), :], dst_ref=spec_ref.at[mrows(f), lanes(0, g)],
            send_sem=s3.at[j], recv_sem=r3.at[j], device_id={"gx": j})

    def forward(j, side):
        f, g = lax.rem(j, lead), j // lead
        place = wide_ref.at[frows(f), lanes(side * kpad, g)]
        return pltpu.make_async_remote_copy(
            src_ref=place, dst_ref=place, send_sem=s4.at[j], recv_sem=r4.at[j], device_id={"gy": peer})

    @pl.loop(1, gx)
    def _(t):
        f = lax.rem(my_lead + t // groups, lead)
        g = lax.rem(my_group + t, groups)
        j = g * lead + f
        syn[blk(j), :] = jnp.dot(xt[blk(j), :], coarse[...], preferred_element_type=f32).astype(bf)
        out2(j).start()

    wide_ref[frows(my_lead), lanes(half * kpad, my_group)] = jnp.dot(
        xt[blk(me), :], coarse[...], preferred_element_type=f32
    ).astype(bf)
    spec_ref[mrows(my_lead), lanes(0, my_group)] = coarse[mrows(me), :]

    @pl.loop(1, gx)
    def _(t):
        out3(lax.rem(me + t, gx)).start()

    forward(me, half).start()

    def low_copy(f):
        return pltpu.make_async_copy(low_ref.at[frows(f), :], low_out.at[frows(f), :], low_sem.at[f])

    @pl.loop(0, lead)
    def _(t):
        f = lax.rem(my_lead + lead - t, lead)

        @pl.loop(0, groups)
        def _(u):
            j = lax.rem(my_group + u, groups) * lead + f

            @pl.when(j != me)
            def _():
                in2(j).wait_recv()
                forward(j, half).start()

        @pl.loop(0, groups)
        def _(u):
            forward(u * lead + f, peer).wait_recv()

        low_ref[frows(f), :] = lax.dot_general(
            wide_ref[frows(f), :], y_ref[...], (((1,), (1,)), ((), ())), preferred_element_type=f32
        ).astype(bf)
        low_copy(f).start()

    @pl.loop(1, gx)
    def _(t):
        j = lax.rem(me + t, gx)
        in3(j).wait_recv()
        out1(j).wait_send()
        out2(j).wait_send()
        out3(j).wait_send()

    @pl.loop(0, gx)
    def _(j):
        forward(j, half).wait_send()

    @pl.loop(0, lead)
    def _(f):
        swap(f).wait_send()
        low_copy(f).wait()


def exchange(gx, lead, x_local, kx, kpad, cols, grid, x_codes, y_codes):
    bf, f32 = jnp.bfloat16, jnp.float32
    rows, codes = lead * x_local, gx * kx
    dma = pltpu.SemaphoreType.DMA
    vmem = pl.BlockSpec(memory_space=pltpu.VMEM)
    y_local = grid.shape[1]
    tall = max(gx * x_local, y_local) // STEP
    return pl.pallas_call(
        functools.partial(exchange_kernel, gx, lead, x_local, kx, kpad, cols),
        out_shape=(
            jax.ShapeDtypeStruct((lead * kx, kpad), bf),
            jax.ShapeDtypeStruct((rows, y_local), bf),
        ),
        in_specs=[pl.BlockSpec(memory_space=pl.ANY), vmem, vmem],
        out_specs=(vmem, pl.BlockSpec(memory_space=pl.ANY)),
        scratch_shapes=[
            pltpu.VMEM((rows, y_local), bf),
            pltpu.VMEM((rows, 2 * kpad), bf),
            pltpu.VMEM((rows, y_local), bf),
            pltpu.VMEM((y_local, 2 * kpad), bf),
            pltpu.VMEM((tall, codes), f32),
            pltpu.VMEM((tall, codes), f32),
            pltpu.VMEM((STEP, codes), f32),
            pltpu.VMEM((STEP, codes), f32),
            pltpu.VMEM((rows, kpad), bf),
            pltpu.VMEM((rows, kpad), bf),
            pltpu.VMEM((rows, kpad), bf),
            pltpu.VMEM((gx * x_local, cols), bf),
            pltpu.VMEM((gx * x_local, codes), bf),
            pltpu.VMEM((cols, codes), f32),
            pltpu.VMEM((codes, cols), bf),
            pltpu.VMEM((gx * x_local, cols), bf),
            dma((lead,)), dma((lead,)),
        ] + [dma((gx,))] * 8 + [dma, dma((lead,))],
        compiler_params=pltpu.CompilerParams(
            collective_id=0, has_side_effects=True, vmem_limit_bytes=60 * 1024 * 1024
        ),
    )(grid, x_codes, y_codes)


def build(gx, gy):
    def local(fields, x_codes, y_codes):
        nf, nz, x_local, y_local = fields.shape
        lead = nf * nz
        ky = y_codes.shape[0] // gy
        kx = x_codes.shape[0] // gx
        unit = 128 * gx // math.gcd(128 * gx, lead)
        if unit > 2 * ky:
            unit = gx // math.gcd(gx, lead)
        kpad = -(-ky // unit) * unit
        cols = lead * kpad // gx
        me_y = lax.axis_index("gy")
        y_first = me_y * y_local
        padded = jnp.pad(y_codes.reshape(gy, ky), ((0, 0), (0, kpad - ky)))
        live = jnp.broadcast_to(jnp.arange(kpad)[None] < ky, (gy, kpad)).reshape(-1)
        grid = fields.reshape(lead * x_local, y_local)
        if gy == 2 and cols % 128 == 0 and cols <= kpad and kpad // cols == gx // lead and x_local % (8 * STEP // gx) == 0 and y_local % (8 * STEP) == 0 and kx % 16 == 0 and gx * kx == gy * kpad:
            padded = jnp.pad(y_codes.reshape(gy, ky), ((0, 0), (0, kpad - ky)), constant_values=-1)
            spec, low = exchange(
                gx, lead, x_local, kx, kpad, cols, grid, x_codes.reshape(1, -1), padded.reshape(1, -1)
            )
            low = low.astype(jnp.float32)
            spectrum = spec.astype(jnp.float32)[:, :ky].reshape(nf, nz, kx, ky)
            return spectrum, low.reshape(nf, nz, x_local, y_local)
        x_tab = mode_table(x_codes, 0, x_local * gx, NX)
        y_tab = mode_table(padded.reshape(-1), y_first, y_local, NY, live)
        part = jnp.dot(grid, y_tab, preferred_element_type=jnp.float32).reshape(lead * x_local, gy, kpad)
        own = lax.dynamic_index_in_dim(part, me_y, 1, keepdims=False)
        for shift in range(1, gy):
            there = lax.rem(me_y + shift, gy)
            block = lax.dynamic_index_in_dim(part, there, 1, keepdims=False).astype(jnp.bfloat16)
            got = lax.ppermute(block, "gy", [(i, (i + shift) % gy) for i in range(gy)])
            own = own + got.astype(jnp.float32)
        send = own.astype(jnp.bfloat16).reshape(lead, x_local, kpad)
        if cols <= kpad:
            def spread(a):
                n = a.shape[1]
                return a.reshape(lead, n, kpad // cols, cols).transpose(0, 2, 1, 3).reshape(gx, n, cols)

            def merge(a):
                n = a.shape[1]
                return a.reshape(lead, kpad // cols, n, cols).transpose(0, 2, 1, 3).reshape(lead, n, kpad)
        else:
            def spread(a):
                n = a.shape[1]
                return a.transpose(1, 0, 2).reshape(n, gx, cols).transpose(1, 0, 2)

            def merge(a):
                n = a.shape[1]
                return a.transpose(1, 0, 2).reshape(n, lead, kpad).transpose(1, 0, 2)
        lines = lax.all_to_all(spread(send), "gx", split_axis=0, concat_axis=0, tiled=True)
        lines = lines.reshape(gx * x_local, cols)
        modes = lax.dot_general(x_tab, lines, (((0,), (0,)), ((), ())), preferred_element_type=jnp.float32)
        coarse = modes.astype(jnp.bfloat16)
        synth = jnp.dot(x_tab, coarse, preferred_element_type=jnp.float32).astype(jnp.bfloat16)
        back = lax.all_to_all(synth.reshape(gx, x_local, cols), "gx", split_axis=0, concat_axis=0, tiled=True)
        spec = lax.all_to_all(coarse.reshape(gx, kx, cols), "gx", split_axis=0, concat_axis=0, tiled=True)
        spectrum = merge(spec)[:, :, :ky].astype(jnp.float32).reshape(nf, nz, kx, ky)
        mine = merge(back).reshape(lead * x_local, kpad)
        y_parts = y_tab.reshape(y_local, gy, kpad)
        whole = jnp.zeros((gy, lead * x_local, kpad), jnp.bfloat16)
        whole = lax.dynamic_update_index_in_dim(whole, mine, me_y, 0)
        for shift in range(1, gy):
            got = lax.ppermute(mine, "gy", [(i, (i + shift) % gy) for i in range(gy)])
            whole = lax.dynamic_update_index_in_dim(whole, got, lax.rem(me_y + gy - shift, gy), 0)
        wide = whole.transpose(1, 0, 2).reshape(lead * x_local, gy * kpad)
        low = lax.dot_general(wide, y_tab, (((1,), (1,)), ((), ())), preferred_element_type=jnp.float32)
        return spectrum, low.reshape(nf, nz, x_local, y_local)

    return local


def solution(mesh):
    return jax.shard_map(
        build(mesh.shape["gx"], mesh.shape["gy"]),
        mesh=mesh,
        in_specs=(P(None, None, "gx", "gy"), P(), P()),
        out_specs=(P(None, None, "gx", "gy"), P(None, None, "gx", "gy")),
        check_vma=False,
    )
```

```python
import functools
import math

import jax
import jax.numpy as jnp
from jax import lax
from jax.experimental import pallas as pl
from jax.experimental.pallas import tpu as pltpu
from jax.sharding import PartitionSpec as P

NX = 3072
NY = 3072
BAND = 512
STEP = 64


def angle(freq, position, length):
    phase = freq[None, :] * position[:, None] % length
    return phase.astype(jnp.float32) * (2.0 * math.pi / length)


def mode_parts(picked, first, amount, length, live=None):
    step = 64 if amount % 64 == 0 else 8
    freq = jnp.where(picked <= BAND, picked, picked - BAND)
    coarse_angle = angle(freq, first + step * jnp.arange(amount // step, dtype=jnp.int32), length)
    fine_angle = angle(freq, jnp.arange(step, dtype=jnp.int32), length)
    norm = jnp.where(picked == 0, 1.0 / math.sqrt(length), math.sqrt(2.0 / length)).astype(jnp.float32)
    if live is not None:
        norm = jnp.where(live, norm, 0.0)
    is_cos = (picked <= BAND)[None, :]
    c, s = jnp.cos(coarse_angle), jnp.sin(coarse_angle)
    first_part = jnp.where(is_cos, c, s) * norm[None, :]
    second_part = jnp.where(is_cos, -s, c) * norm[None, :]
    fc, fs = jnp.cos(fine_angle), jnp.sin(fine_angle)
    return lax.optimization_barrier((first_part, second_part, fc, fs))


def mode_table(picked, first, amount, length, live=None):
    first_part, second_part, fc, fs = mode_parts(picked, first, amount, length, live)
    table = first_part[:, None, :] * fc[None] + second_part[:, None, :] * fs[None]
    return table.astype(jnp.bfloat16).reshape(amount, picked.shape[0])


def al(v, m):
    return pl.multiple_of(v, m)


def turn(freq, position, shift, length):
    product = freq * position
    quarter = jnp.floor(product * (4.0 / length) + 0.5)
    x = (product * 4.0 - quarter * length) * (2.0 * math.pi / (4 * length))
    x2 = x * x
    s = x + x * x2 * (-1 / 6 + x2 * (1 / 120 + x2 * (-1 / 5040 + x2 * (1 / 362880))))
    c = 1.0 + x2 * (-0.5 + x2 * (1 / 24 + x2 * (-1 / 720 + x2 * (1 / 40320))))
    quarter = quarter - shift
    q = quarter - 4.0 * jnp.floor(quarter * 0.25)
    odd = (q == 1.0) | (q == 3.0)
    cos_value, sin_value = jnp.where(odd, s, c), jnp.where(odd, c, s)
    cos_value = jnp.where((q == 1.0) | (q == 2.0), -cos_value, cos_value)
    return cos_value, jnp.where(q >= 2.0, -sin_value, sin_value)


def make_table(code_ref, first, length, table, ta, tb, fc, fs):
    amount, codes = table.shape
    f32 = jnp.float32
    code = code_ref[...]
    freq = jnp.where(code <= BAND, code, code - BAND).astype(f32)
    shift = jnp.where(code <= BAND, 0, 1).astype(f32)
    norm = jnp.where(code == 0, 1.0 / math.sqrt(length), math.sqrt(2.0 / length)).astype(f32)
    norm = jnp.where(code < 0, 0.0, norm)
    row = lax.broadcasted_iota(jnp.int32, (8, codes), 0)

    @pl.loop(0, amount // STEP // 8)
    def _(i):
        c, s = turn(freq, (first + (row + i * 8) * STEP).astype(f32), shift, length)
        ta[pl.ds(al(i * 8, 8), 8), :] = c * norm
        tb[pl.ds(al(i * 8, 8), 8), :] = s * norm

    @pl.loop(0, STEP // 8)
    def _(i):
        c, s = turn(freq, (row + i * 8).astype(f32), 0.0, length)
        fc[pl.ds(al(i * 8, 8), 8), :] = c
        fs[pl.ds(al(i * 8, 8), 8), :] = s

    @pl.loop(0, amount // STEP)
    def _(h):
        table[pl.ds(al(h * STEP, STEP), STEP), :] = (
            ta[pl.ds(h, 1), :] * fc[...] - tb[pl.ds(h, 1), :] * fs[...]
        ).astype(jnp.bfloat16)


def exchange_kernel(
    gx, lead, x_local, kx, kpad, cols,
    grid_in, xcode_ref, ycode_ref, spec_ref, low_out,
    grid_ref, wide_ref, low_ref, y_ref, ta, tb, fc, fs, other, inc, part, lines, xt, acc, coarse, syn,
    gs, gr, s1, r1, s2, r2, s3, r3, s4, r4, grid_sem, low_sem,
):
    me = lax.axis_index("gx")
    half = lax.axis_index("gy")
    peer = 1 - half
    groups = gx // lead
    my_group, my_lead = me // lead, lax.rem(me, lead)
    bf, f32 = jnp.bfloat16, jnp.float32

    grid_copy = pltpu.make_async_copy(grid_in, grid_ref, grid_sem)
    grid_copy.start()
    barrier = pltpu.get_barrier_semaphore()
    pl.semaphore_signal(barrier, inc=1, device_id={"gy": peer})

    @pl.loop(1, gx)
    def _(t):
        pl.semaphore_signal(barrier, inc=1, device_id={"gx": lax.rem(me + t, gx)})

    def frows(f):
        return pl.ds(al(f * x_local, x_local), x_local)

    def blk(j):
        return pl.ds(al(j * x_local, x_local), x_local)

    def lanes(base, g):
        return pl.ds(al(base + g * cols, cols), cols)

    def y_half(side):
        span = pl.ds(al(side * kpad, kpad), kpad)
        narrow = [r.at[:, pl.ds(0, kpad)] for r in (ta, tb, fc, fs)]
        make_table(ycode_ref.at[:, span], half * y_ref.shape[0], NY, y_ref.at[:, span], *narrow)

    y_half(peer)
    grid_copy.wait()

    @pl.loop(0, lead)
    def _(t):
        f = lax.rem(my_lead + t, lead)
        other[frows(f), :] = jnp.dot(
            grid_ref[frows(f), :], y_ref[:, pl.ds(al(peer * kpad, kpad), kpad)], preferred_element_type=f32
        ).astype(bf)

    pl.semaphore_wait(barrier, gx)

    def swap(f):
        return pltpu.make_async_remote_copy(
            src_ref=other.at[frows(f), :], dst_ref=inc.at[frows(f), :], send_sem=gs.at[f], recv_sem=gr.at[f],
            device_id={"gy": peer})

    @pl.loop(0, lead)
    def _(t):
        swap(lax.rem(my_lead + t, lead)).start()

    y_half(half)

    def out1(j):
        f, g = lax.rem(j, lead), j // lead
        return pltpu.make_async_remote_copy(
            src_ref=part.at[frows(f), lanes(0, g)], dst_ref=lines.at[blk(me), :], send_sem=s1.at[j],
            recv_sem=r1.at[me], device_id={"gx": j})

    def in1(j):
        return pltpu.make_async_remote_copy(
            src_ref=part.at[frows(0), lanes(0, 0)], dst_ref=lines.at[blk(j), :], send_sem=s1.at[j],
            recv_sem=r1.at[j], device_id={"gx": j})

    @pl.loop(0, lead)
    def _(t):
        f = lax.rem(my_lead + t, lead)
        own = jnp.dot(
            grid_ref[frows(f), :], y_ref[:, pl.ds(al(half * kpad, kpad), kpad)], preferred_element_type=f32
        )
        swap(f).wait_recv()
        part[frows(f), :] = (own + inc[frows(f), :].astype(f32)).astype(bf)

        @pl.loop(0, groups)
        def _(u):
            g = lax.rem(my_group + u, groups)
            j = g * lead + f

            @pl.when(j != me)
            def _():
                out1(j).start()

    lines[blk(me), :] = part[frows(my_lead), lanes(0, my_group)]

    make_table(xcode_ref, 0, NX, xt, ta, tb, fc, fs)
    acc[...] = jnp.zeros_like(acc)

    @pl.loop(0, gx)
    def _(t):
        f = lax.rem(my_lead + lead - t // groups, lead)
        g = lax.rem(my_group + t, groups)
        j = g * lead + f

        @pl.when(j != me)
        def _():
            in1(j).wait_recv()

        acc[...] += jnp.dot(lines[blk(j), :].T, xt[blk(j), :], preferred_element_type=f32)

    coarse[...] = acc[...].T.astype(bf)

    def out2(j):
        return pltpu.make_async_remote_copy(
            src_ref=syn.at[blk(j), :], dst_ref=wide_ref.at[frows(my_lead), lanes(half * kpad, my_group)],
            send_sem=s2.at[j], recv_sem=r2.at[me], device_id={"gx": j})

    def in2(j):
        f, g = lax.rem(j, lead), j // lead
        return pltpu.make_async_remote_copy(
            src_ref=syn.at[blk(j), :], dst_ref=wide_ref.at[frows(f), lanes(half * kpad, g)],
            send_sem=s2.at[j], recv_sem=r2.at[j], device_id={"gx": j})

    def mrows(j):
        return pl.ds(al(j * kx, kx), kx)

    def out3(j):
        return pltpu.make_async_remote_copy(
            src_ref=coarse.at[mrows(j), :], dst_ref=spec_ref.at[mrows(my_lead), lanes(0, my_group)],
            send_sem=s3.at[j], recv_sem=r3.at[me], device_id={"gx": j})

    def in3(j):
        f, g = lax.rem(j, lead), j // lead
        return pltpu.make_async_remote_copy(
            src_ref=coarse.at[mrows(j), :], dst_ref=spec_ref.at[mrows(f), lanes(0, g)],
            send_sem=s3.at[j], recv_sem=r3.at[j], device_id={"gx": j})

    def forward(j, side):
        f, g = lax.rem(j, lead), j // lead
        place = wide_ref.at[frows(f), lanes(side * kpad, g)]
        return pltpu.make_async_remote_copy(
            src_ref=place, dst_ref=place, send_sem=s4.at[j], recv_sem=r4.at[j], device_id={"gy": peer})

    @pl.loop(1, gx)
    def _(t):
        f = lax.rem(my_lead + t // groups, lead)
        g = lax.rem(my_group + t, groups)
        j = g * lead + f
        syn[blk(j), :] = jnp.dot(xt[blk(j), :], coarse[...], preferred_element_type=f32).astype(bf)
        out2(j).start()

    wide_ref[frows(my_lead), lanes(half * kpad, my_group)] = jnp.dot(
        xt[blk(me), :], coarse[...], preferred_element_type=f32
    ).astype(bf)
    spec_ref[mrows(my_lead), lanes(0, my_group)] = coarse[mrows(me), :]

    @pl.loop(1, gx)
    def _(t):
        out3(lax.rem(me + t, gx)).start()

    forward(me, half).start()

    def low_copy(f):
        return pltpu.make_async_copy(low_ref.at[frows(f), :], low_out.at[frows(f), :], low_sem.at[f])

    @pl.loop(0, lead)
    def _(t):
        f = lax.rem(my_lead + lead - t, lead)

        @pl.loop(0, groups)
        def _(u):
            j = lax.rem(my_group + u, groups) * lead + f

            @pl.when(j != me)
            def _():
                in2(j).wait_recv()
                forward(j, half).start()

        @pl.loop(0, groups)
        def _(u):
            forward(u * lead + f, peer).wait_recv()

        low_ref[frows(f), :] = lax.dot_general(
            wide_ref[frows(f), :], y_ref[...], (((1,), (1,)), ((), ())), preferred_element_type=f32
        ).astype(bf)
        low_copy(f).start()

    @pl.loop(1, gx)
    def _(t):
        j = lax.rem(me + t, gx)
        in3(j).wait_recv()
        out1(j).wait_send()
        out2(j).wait_send()
        out3(j).wait_send()

    @pl.loop(0, gx)
    def _(j):
        forward(j, half).wait_send()

    @pl.loop(0, lead)
    def _(f):
        swap(f).wait_send()
        low_copy(f).wait()


def exchange(gx, lead, x_local, kx, kpad, cols, grid, x_codes, y_codes):
    bf, f32 = jnp.bfloat16, jnp.float32
    rows, codes = lead * x_local, gx * kx
    dma = pltpu.SemaphoreType.DMA
    vmem = pl.BlockSpec(memory_space=pltpu.VMEM)
    y_local = grid.shape[1]
    tall = max(gx * x_local, y_local) // STEP
    return pl.pallas_call(
        functools.partial(exchange_kernel, gx, lead, x_local, kx, kpad, cols),
        out_shape=(
            jax.ShapeDtypeStruct((lead * kx, kpad), bf),
            jax.ShapeDtypeStruct((rows, y_local), bf),
        ),
        in_specs=[pl.BlockSpec(memory_space=pl.ANY), vmem, vmem],
        out_specs=(vmem, pl.BlockSpec(memory_space=pl.ANY)),
        scratch_shapes=[
            pltpu.VMEM((rows, y_local), bf),
            pltpu.VMEM((rows, 2 * kpad), bf),
            pltpu.VMEM((rows, y_local), bf),
            pltpu.VMEM((y_local, 2 * kpad), bf),
            pltpu.VMEM((tall, codes), f32),
            pltpu.VMEM((tall, codes), f32),
            pltpu.VMEM((STEP, codes), f32),
            pltpu.VMEM((STEP, codes), f32),
            pltpu.VMEM((rows, kpad), bf),
            pltpu.VMEM((rows, kpad), bf),
            pltpu.VMEM((rows, kpad), bf),
            pltpu.VMEM((gx * x_local, cols), bf),
            pltpu.VMEM((gx * x_local, codes), bf),
            pltpu.VMEM((cols, codes), f32),
            pltpu.VMEM((codes, cols), bf),
            pltpu.VMEM((gx * x_local, cols), bf),
            dma((lead,)), dma((lead,)),
        ] + [dma((gx,))] * 8 + [dma, dma((lead,))],
        compiler_params=pltpu.CompilerParams(
            collective_id=0, has_side_effects=True, vmem_limit_bytes=60 * 1024 * 1024
        ),
    )(grid, x_codes, y_codes)


def build(gx, gy):
    def local(fields, x_codes, y_codes):
        nf, nz, x_local, y_local = fields.shape
        lead = nf * nz
        ky = y_codes.shape[0] // gy
        kx = x_codes.shape[0] // gx
        unit = 128 * gx // math.gcd(128 * gx, lead)
        if unit > 2 * ky:
            unit = gx // math.gcd(gx, lead)
        kpad = -(-ky // unit) * unit
        cols = lead * kpad // gx
        me_y = lax.axis_index("gy")
        y_first = me_y * y_local
        padded = jnp.pad(y_codes.reshape(gy, ky), ((0, 0), (0, kpad - ky)))
        live = jnp.broadcast_to(jnp.arange(kpad)[None] < ky, (gy, kpad)).reshape(-1)
        grid = fields.reshape(lead * x_local, y_local)
        if gy == 2 and cols % 128 == 0 and cols <= kpad and kpad // cols == gx // lead and x_local % (8 * STEP // gx) == 0 and y_local % (8 * STEP) == 0 and kx % 16 == 0 and gx * kx == gy * kpad:
            padded = jnp.pad(y_codes.reshape(gy, ky), ((0, 0), (0, kpad - ky)), constant_values=-1)
            spec, low = exchange(
                gx, lead, x_local, kx, kpad, cols, grid, x_codes.reshape(1, -1), padded.reshape(1, -1)
            )
            low = low.astype(jnp.float32)
            spectrum = spec.astype(jnp.float32)[:, :ky].reshape(nf, nz, kx, ky)
            return spectrum, low.reshape(nf, nz, x_local, y_local)
        x_tab = mode_table(x_codes, 0, x_local * gx, NX)
        y_tab = mode_table(padded.reshape(-1), y_first, y_local, NY, live)
        part = jnp.dot(grid, y_tab, preferred_element_type=jnp.float32).reshape(lead * x_local, gy, kpad)
        own = lax.dynamic_index_in_dim(part, me_y, 1, keepdims=False)
        for shift in range(1, gy):
            there = lax.rem(me_y + shift, gy)
            block = lax.dynamic_index_in_dim(part, there, 1, keepdims=False).astype(jnp.bfloat16)
            got = lax.ppermute(block, "gy", [(i, (i + shift) % gy) for i in range(gy)])
            own = own + got.astype(jnp.float32)
        send = own.astype(jnp.bfloat16).reshape(lead, x_local, kpad)
        if cols <= kpad:
            def spread(a):
                n = a.shape[1]
                return a.reshape(lead, n, kpad // cols, cols).transpose(0, 2, 1, 3).reshape(gx, n, cols)

            def merge(a):
                n = a.shape[1]
                return a.reshape(lead, kpad // cols, n, cols).transpose(0, 2, 1, 3).reshape(lead, n, kpad)
        else:
            def spread(a):
                n = a.shape[1]
                return a.transpose(1, 0, 2).reshape(n, gx, cols).transpose(1, 0, 2)

            def merge(a):
                n = a.shape[1]
                return a.transpose(1, 0, 2).reshape(n, lead, kpad).transpose(1, 0, 2)
        lines = lax.all_to_all(spread(send), "gx", split_axis=0, concat_axis=0, tiled=True)
        lines = lines.reshape(gx * x_local, cols)
        modes = lax.dot_general(x_tab, lines, (((0,), (0,)), ((), ())), preferred_element_type=jnp.float32)
        coarse = modes.astype(jnp.bfloat16)
        synth = jnp.dot(x_tab, coarse, preferred_element_type=jnp.float32).astype(jnp.bfloat16)
        back = lax.all_to_all(synth.reshape(gx, x_local, cols), "gx", split_axis=0, concat_axis=0, tiled=True)
        spec = lax.all_to_all(coarse.reshape(gx, kx, cols), "gx", split_axis=0, concat_axis=0, tiled=True)
        spectrum = merge(spec)[:, :, :ky].astype(jnp.float32).reshape(nf, nz, kx, ky)
        mine = merge(back).reshape(lead * x_local, kpad)
        y_parts = y_tab.reshape(y_local, gy, kpad)
        whole = jnp.zeros((gy, lead * x_local, kpad), jnp.bfloat16)
        whole = lax.dynamic_update_index_in_dim(whole, mine, me_y, 0)
        for shift in range(1, gy):
            got = lax.ppermute(mine, "gy", [(i, (i + shift) % gy) for i in range(gy)])
            whole = lax.dynamic_update_index_in_dim(whole, got, lax.rem(me_y + gy - shift, gy), 0)
        wide = whole.transpose(1, 0, 2).reshape(lead * x_local, gy * kpad)
        low = lax.dot_general(wide, y_tab, (((1,), (1,)), ((), ())), preferred_element_type=jnp.float32)
        return spectrum, low.reshape(nf, nz, x_local, y_local)

    return local


def solution(mesh):
    return jax.shard_map(
        build(mesh.shape["gx"], mesh.shape["gy"]),
        mesh=mesh,
        in_specs=(P(None, None, "gx", "gy"), P(), P()),
        out_specs=(P(None, None, "gx", "gy"), P(None, None, "gx", "gy")),
        check_vma=False,
    )
```
